32 devices in a mesh: pair: 8 (over y, x, core), aux: 4 (over z).
Axes of the slice: x: 2, y: 2, z: 4, core: 2. Of those that a mesh axis runs over, the one named last changes fastest.
Arguments:
- integrals: bfloat16 [512, 256, 64], P(('pair', 'aux')), may hold values from -6 to 6
- amplitudes: bfloat16 [512, 64, 64], P(('pair', 'aux')), may hold values from -0.75 to 0.75
- pno_density: bfloat16 [512, 64, 64], P(('pair', 'aux')), may hold values from -6 to 6
- pno_coef: bfloat16 [512, 256, 64], P(('pair', 'aux')), may hold values from -0.75 to 0.75
- pao_blocks: int32 [512, 2], P(('pair', 'aux')), may hold values from 0 to 5, all different within a row
- aux_slice: int32 [512, 2], P(('pair', 'aux')), may hold values from 0 to 3, all different within a row; in each aligned block of 16 rows (0 to 15, 16 to 31, ...) at most 16 rows name the same one
- aux_offset: int32 [512, 2], P(('pair', 'aux')), may hold values from 0 to 3
Outputs:
- aux_density: float32 [2048, 768], P('aux', 'pair')
- virtual_density: float32 [768, 768], P('aux', 'pair')
The draws below stay inside these ranges and needn't reach their ends.
Inputs may be any that keep to these rules, and one draw needn't show every extreme that they name: `pao_blocks`: the 2 blocks of a pair are different. `aux_slice`: the 2 slices of a pair are different; among the pairs of one device no slice is named more than 16 times, and in every draw some device names some slice exactly 16 times.
All inputs are finite; a program needn't handle non-finite values.
Results may differ from the reference program's by a relative error of at most 0.0041.
Values may be sent and summed in bfloat16 or wider, within the bound.
A program may use at most 64 MiB of HBM per device.

```python
import math
import jax
import jax.numpy as jnp
import numpy as np
from jax import lax

NPNO = 64
ABLK = 128
PBLK = 128
DOMB = 2
ADOM = 2
NBLK = 6
ABPO = 4
PAIR_DEV = 16
PAIRS = 512
CAP = 16
N_PAIR = 8
N_AUX = 4


def touch_ends(drawn, rng, least, top_value):
    place = [jax.random.randint(jax.random.fold_in(rng, axis), (), 0, length) for axis, length in enumerate(drawn.shape)]
    longest = drawn.shape.index(max(drawn.shape))
    next_to = place[:longest] + [(place[longest] + 1) % drawn.shape[longest]] + place[longest + 1:]
    return drawn.at[tuple(place)].set(least).at[tuple(next_to)].set(top_value)


def block_levels(own_key, dims, shards, low, largest):
    def one(position, shards_of):
        heights = jax.random.uniform(jax.random.fold_in(jax.random.fold_in(own_key, 6), position), (shards_of,), jnp.float32, low / len(shards), largest / len(shards))
        return jnp.repeat(jnp.exp(heights), dims[position] // shards_of).reshape((-1,) + (1,) * (len(dims) - position - 1))

    factor_of = one(*shards[0])
    for cut in shards[1:]:
        factor_of = factor_of * one(*cut)
    return factor_of


def different_ones(stream_key, rows, count, top, lift):
    order = jax.random.permutation(jax.random.fold_in(stream_key, 1), count)
    pull = order
    for power in range(3):
        pull = pull * pull // count
    pull = pull * lift // count
    tickets = jax.random.randint(jax.random.fold_in(stream_key, 2), (rows, count), 0, 4096) + pull
    holders = jax.random.permutation(jax.random.fold_in(stream_key, 3), rows)[jnp.arange(count) % rows]
    tickets = jnp.where(jnp.arange(rows)[:, None] == holders[None, :], 1 << 14, tickets)
    score = tickets * count + jnp.arange(count)
    return lax.top_k(score.astype(jnp.int32), top)[1].astype(jnp.int32)


def routed_block(rng, own, number, rows, number_of, top, reach, slope):
    ranking = jax.random.permutation(rng, number_of)
    heavy_load, usual = load_shares(number_of, rows * top, reach, slope, True), load_shares(number_of, rows * top, reach, slope, False)
    places = jnp.arange(number_of)

    def named(sizes, offset_by):
        used = int((sizes > 0).sum())
        fixed = max(1, used // 4)
        moved = fixed + (places - fixed + offset_by * (used - fixed)) % max(1, number_of - fixed)
        return jnp.zeros((number_of,), jnp.int32).at[ranking[jnp.where(places < fixed, places, moved)]].set(jnp.asarray(sizes, jnp.int32))

    sizes = jnp.where(number % 4 == 0, named(heavy_load, number // 4), named(usual, number - number // 4 - 1))
    mixed = jax.random.permutation(jax.random.fold_in(own, 3), number_of)
    source_of, taker = mixed[0:number_of // 2 * 2:2], mixed[1:number_of // 2 * 2:2]
    room = jnp.minimum(sizes[source_of] - 1, reach - sizes[taker]) // 2
    room = jnp.where((source_of == ranking[0]) | (taker == ranking[0]) | (sizes[taker] == 0), 0, jnp.maximum(room, 0))
    moved = jax.random.randint(jax.random.fold_in(own, 4), (number_of // 2,), 0, 1 << 20) % (room + 1)
    sizes = sizes.at[source_of].add(-moved).at[taker].add(moved)
    members = jnp.searchsorted(jnp.cumsum(sizes), jnp.arange(rows * top), side="right").astype(jnp.int32)
    listing = members.reshape(top, rows).T
    listing = listing[jax.random.permutation(jax.random.fold_in(own, 1), rows)]
    offset_by = jax.random.randint(jax.random.fold_in(own, 2), (rows, 1), 0, top)
    return jnp.take_along_axis(listing, (jnp.arange(top)[None, :] + offset_by) % top, axis=1)


def load_shares(number_of, total, bound, skew, full):
    loads = [(1 << 20) // math.isqrt(grade ** skew) + 1 for grade in range(1, number_of + 1)]
    largest = bound if full else min(bound, max(-(-total // number_of), total * loads[0] // sum(loads)))
    least = 1 if total - largest >= number_of - 1 else 0
    holding, surplus = [largest] + [least] * (number_of - 1), total - largest - least * (number_of - 1)
    while surplus > 0:
        free = [i for i in range(1, number_of) if holding[i] < largest] or [i for i in range(1, number_of) if holding[i] < bound]
        whole, left = sum([loads[i] for i in free]), surplus
        for i in free:
            addition = min(bound - holding[i], max(1, left * loads[i] // whole), surplus)
            holding[i] = holding[i] + addition
            surplus = surplus - addition
    return np.array(holding)


def scatter_about(own_key, shape, spread, most, cuts=(), kind=jnp.bfloat16):
    values = spread * jax.random.normal(own_key, shape, jnp.float32)
    if cuts:
        values = values * block_levels(own_key, shape, cuts, -0.22, 0.18)
    return jnp.clip(values, -most, most).astype(kind)


def setup_inputs(seed: int = 0) -> dict:
    streams_of = jax.random.split(jax.random.key(seed), 8)
    integrals = scatter_about(streams_of[0], (PAIRS, ADOM * ABLK, NPNO), 1.0, 6.0, ((0, 32),))
    amplitudes = scatter_about(streams_of[1], (PAIRS, NPNO, NPNO), NPNO ** -0.5, 0.75, ((0, 32),))
    pno_density = scatter_about(streams_of[2], (PAIRS, NPNO, NPNO), 1.0, 6.0, ((0, 32),))
    pno_coef = scatter_about(streams_of[3], (PAIRS, DOMB * PBLK, NPNO), NPNO ** -0.5, 0.75, ((0, 32),))
    pao_blocks = different_ones(streams_of[4], PAIRS, NBLK, DOMB, 2730)
    aux_slice_keys = jax.random.split(jax.random.fold_in(streams_of[5], 1), PAIRS // PAIR_DEV)
    aux_slice_turns = jax.random.permutation(jax.random.fold_in(streams_of[5], 3), PAIRS // PAIR_DEV)
    aux_slice = jax.vmap(lambda own, number: routed_block(jax.random.fold_in(streams_of[5], 2), own, number, PAIR_DEV, N_AUX, ADOM, CAP, 2))(aux_slice_keys, aux_slice_turns).reshape((PAIRS, ADOM))
    aux_offset = touch_ends(jax.random.randint(streams_of[6], (PAIRS, ADOM), 0, ABPO), jax.random.fold_in(streams_of[6], 1), 0, ABPO - 1).astype(jnp.int32)
    return dict(integrals=integrals, amplitudes=amplitudes, pno_density=pno_density, pno_coef=pno_coef, pao_blocks=pao_blocks, aux_slice=aux_slice, aux_offset=aux_offset)


def reference(integrals, amplitudes, pno_density, pno_coef, pao_blocks, aux_slice, aux_offset):
    block_pairs = PAIR_DEV * N_AUX
    out_scale = 1.0 / math.sqrt(PAIR_DEV * N_PAIR)

    def add_block(carry, block_index):
        gamma_acc, virt_acc = carry
        first = (block_index * block_pairs).astype(jnp.int32)

        def take(array):
            return lax.dynamic_slice_in_dim(array, first, block_pairs, 0)
        block_ints = take(integrals).astype(jnp.float32)
        block_amps = take(amplitudes).astype(jnp.float32)
        block_dens = take(pno_density).astype(jnp.float32)
        block_coef = take(pno_coef).astype(jnp.float32)
        block_pao = take(pao_blocks)
        block_rows = take(aux_slice) * ABPO + take(aux_offset)
        three_index = jnp.einsum('pqr,prs->pqs', block_ints, block_amps).astype(jnp.bfloat16)
        three_index = lax.optimization_barrier(three_index).astype(jnp.float32)
        pao_pieces = jnp.einsum('pqs,pys->pqy', three_index, block_coef).astype(jnp.bfloat16)
        pao_pieces = lax.optimization_barrier(pao_pieces).astype(jnp.float32)
        pieces = pao_pieces.reshape(block_pairs, ADOM, ABLK, DOMB, PBLK).transpose(0, 1, 3, 2, 4)
        gamma_acc = gamma_acc.at[block_rows[:, :, None], :, block_pao[:, None, :], :].add(pieces)
        weighted = jnp.einsum('pyr,prs->pys', block_coef, block_dens).astype(jnp.bfloat16)
        weighted = lax.optimization_barrier(weighted).astype(jnp.float32)
        pair_density = jnp.einsum('pys,pzs->pyz', weighted, block_coef)
        pair_density = pair_density.reshape(block_pairs, DOMB, PBLK, DOMB, PBLK).transpose(0, 1, 3, 2, 4)
        virt_acc = virt_acc.at[block_pao[:, :, None], :, block_pao[:, None, :], :].add(pair_density)
        return ((gamma_acc, virt_acc), None)
    gamma_init = jnp.zeros((N_AUX * ABPO, ABLK, NBLK, PBLK), jnp.float32)
    virt_init = jnp.zeros((NBLK, PBLK, NBLK, PBLK), jnp.float32)
    (gamma_acc, virt_acc), _ = lax.scan(add_block, (gamma_init, virt_init), jnp.arange(N_PAIR, dtype=jnp.int32))
    aux_density = gamma_acc.reshape(N_AUX * ABPO * ABLK, NBLK * PBLK) * out_scale
    virtual_density = virt_acc.reshape(NBLK * PBLK, NBLK * PBLK) * out_scale
    return (aux_density, virtual_density)
```

```python
import functools
import math

import jax
import jax.numpy as jnp
from jax import lax
from jax.experimental import pallas as pl
from jax.experimental.pallas import tpu as pltpu
from jax.sharding import PartitionSpec as P

NBLK = 6
ABPO = 4
MESH = pl.DeviceIdType.MESH
TILE = 128
SUB = 16


def by_collectives(integrals, amplitudes, pno_density, pno_coef, pao_blocks, aux_slice, aux_offset):
    n_pair = lax.axis_size("pair")
    n_aux = lax.axis_size("aux")
    pair_count, domain_rows, pno_rank = pno_coef.shape
    aux_dom = aux_slice.shape[1]
    pao_dom = pao_blocks.shape[1]
    pao_block = domain_rows // pao_dom
    aux_block = integrals.shape[1] // aux_dom
    ao_count = NBLK * pao_block
    capacity = max(2, 2 * pair_count * aux_dom // n_aux)
    out_scale = 1.0 / math.sqrt(pair_count * n_pair)
    slot_count = pair_count * aux_dom
    three_index = jnp.einsum(
        "pqr,prs->pqs", integrals, amplitudes, preferred_element_type=jnp.float32
    ).astype(jnp.bfloat16)
    owners = aux_slice.reshape(slot_count)
    owner_hot = (owners[:, None] == jnp.arange(n_aux, dtype=jnp.int32)[None, :]).astype(jnp.int32)
    before = jnp.cumsum(owner_hot, 0) - owner_hot
    slot_rank = jnp.sum(before * owner_hot, 1)
    target = owners * capacity + slot_rank
    routing = jnp.arange(n_aux * capacity, dtype=jnp.int32)[:, None] == target[None, :]
    labels = (
        jnp.concatenate(
            [aux_offset.reshape(slot_count, 1), jnp.repeat(pao_blocks, aux_dom, axis=0)], 1
        )
        + 1
    )
    label_buffer = (jnp.dot(routing.astype(jnp.int32), labels) - 1).reshape(
        n_aux, capacity, 1 + pao_dom
    )
    routing_bf = routing.astype(jnp.bfloat16)
    index_flat = three_index.reshape(slot_count, aux_block * pno_rank)
    index_buffer = jnp.dot(routing_bf, index_flat, preferred_element_type=jnp.float32).astype(
        jnp.bfloat16
    )
    index_buffer = index_buffer.reshape(n_aux, capacity, aux_block, pno_rank)
    pair_routing = (
        routing.reshape(n_aux * capacity, pair_count, aux_dom).sum(-1).astype(jnp.bfloat16)
    )
    coef_flat = pno_coef.reshape(pair_count, domain_rows * pno_rank)
    coef_buffer = jnp.dot(pair_routing, coef_flat, preferred_element_type=jnp.float32).astype(
        jnp.bfloat16
    )
    coef_buffer = coef_buffer.reshape(n_aux, capacity, domain_rows, pno_rank)
    index_part = lax.all_to_all(index_buffer, "aux", split_axis=0, concat_axis=0, tiled=True)
    coef_part = lax.all_to_all(coef_buffer, "aux", split_axis=0, concat_axis=0, tiled=True)
    label_part = lax.all_to_all(label_buffer, "aux", split_axis=0, concat_axis=0, tiled=True)
    back = jnp.einsum(
        "ncxr,ncyr->ncxy", index_part, coef_part, preferred_element_type=jnp.float32
    ).astype(jnp.bfloat16)
    got_labels = label_part
    received_count = n_aux * capacity
    pieces = back.reshape(received_count, aux_block, pao_dom, pao_block)
    got_labels = got_labels.reshape(received_count, 1 + pao_dom)
    offset_hot = got_labels[:, 0:1] == jnp.arange(ABPO, dtype=jnp.int32)[None, :]
    column_hot = got_labels[:, 1:, None] == jnp.arange(NBLK, dtype=jnp.int32)[None, None, :]
    placement = (offset_hot[:, None, :, None] & column_hot[:, :, None, :]).astype(jnp.bfloat16)
    gamma_part = jnp.einsum(
        "sxhy,shok->oxky", pieces, placement, preferred_element_type=jnp.float32
    )
    gamma_part = gamma_part.reshape(ABPO * aux_block, ao_count)
    aux_density = lax.psum_scatter(gamma_part, "pair", scatter_dimension=1, tiled=True) * out_scale
    weighted = jnp.einsum(
        "pyr,prs->pys", pno_coef, pno_density, preferred_element_type=jnp.float32
    ).astype(jnp.bfloat16)
    block_hot = (pao_blocks[:, :, None] == jnp.arange(NBLK, dtype=jnp.int32)[None, None, :]).astype(
        jnp.bfloat16
    )
    weighted_rows = jnp.einsum(
        "pak,paxr->kxpr",
        block_hot,
        weighted.reshape(pair_count, pao_dom, pao_block, pno_rank),
        preferred_element_type=jnp.float32,
    ).astype(jnp.bfloat16)
    weighted_rows = weighted_rows.reshape(ao_count, pair_count * pno_rank)
    coef_rows = jnp.einsum(
        "pak,paxr->kxpr",
        block_hot,
        pno_coef.reshape(pair_count, pao_dom, pao_block, pno_rank),
        preferred_element_type=jnp.float32,
    ).astype(jnp.bfloat16)
    coef_rows = coef_rows.reshape(ao_count, pair_count * pno_rank)
    virt_part = lax.dot_general(
        weighted_rows, coef_rows, (((1,), (1,)), ((), ())), preferred_element_type=jnp.float32
    )
    row_owned = lax.psum_scatter(virt_part, "aux", scatter_dimension=0, tiled=True)
    virtual_density = lax.psum_scatter(row_owned, "pair", scatter_dimension=1, tiled=True)
    return (aux_density, virtual_density * out_scale)


TILES = (("virt", 0, 0), ("virt", 0, 1), ("virt", 0, 2), ("aux", "far", 0), ("aux", "far", 1),
         ("aux", "early", 0), ("aux", "late", 0), ("aux", "early", 1), ("aux", "late", 1), ("aux", "own", 0), ("aux", "own", 1))
WIDE = 2 * TILE
RECVS = 3 * len(TILES) + 9
SENDS = 6


def kernel(scale, ints_in, amps_in, dens_in, coef_in, pao_in, aux_in, off_in, gamma, virt,
           ints, amps, dens, coef, pao, aux, off, labels, coef2, tri2, wei2, lhs, rhs, own, c_send, c_recv,
           s1_send, s1_recv, s2_send, s2_recv, keep1, keep2,
           p_send, p_recv, f_send, f_recv, v_send, v_recv, v_sum, flat, turned, load_sems, send_sems, recv_sems):
    pairs, rank, rows = coef.shape
    couples = pairs // 2
    shard = gamma.shape[0]
    part = shard // 2
    half_rows = 4 * shard
    f32, bf16 = jnp.float32, jnp.bfloat16
    p = lax.axis_index("pair")
    z = lax.axis_index("aux")
    c, x, y = p % 2, (p // 2) % 2, p // 4
    z0, z1 = z % 2, z // 2
    core = (p + 1 - 2 * c, z)
    xdev = (p + 2 - 4 * x, z)
    ydev = (p + 4 - 8 * y, z)
    flips = (z, z + 1 - 2 * z0, z + 2 - 4 * z1, 3 - z)
    at_end = 1 - (z0 + z1) % 2
    early, late = 1 + at_end, 2 - at_end
    flip_of = {"own": 0, "far": 3, "early": early, "late": late}
    owner_of = {"own": z, "far": flips[3], "early": flips[1] + at_end * (flips[2] - flips[1]),
                "late": flips[2] + at_end * (flips[1] - flips[2])}

    loads = [
        pltpu.make_async_copy(src, dst, load_sems.at[n])
        for n, (src, dst) in enumerate((
            (pao_in, pao), (coef_in, coef), (dens_in, dens), (amps_in, amps), (ints_in, ints), (aux_in, aux), (off_in, off)))
    ]
    for load in loads:
        load.start()

    barrier = pltpu.get_barrier_semaphore()
    for dev in (core, xdev, ydev) + tuple((p, flips[n]) for n in (1, 2, 3)):
        pl.semaphore_signal(barrier, inc=1, device_id=dev, device_id_type=MESH)

    def send(src, dst, family, slot, dev):
        pltpu.make_async_remote_copy(
            src_ref=src, dst_ref=dst, send_sem=send_sems.at[family], recv_sem=recv_sems.at[slot],
            device_id=dev, device_id_type=MESH).start()

    def arrived(ref, slot):
        pltpu.make_async_copy(ref, ref, recv_sems.at[slot]).wait()

    zero = jnp.zeros((rank, rank), bf16)

    def mixed(ref, q, both):
        diag = jnp.concatenate(
            [jnp.concatenate([ref[2 * q], zero], 1), jnp.concatenate([zero, ref[2 * q + 1]], 1)], 0)
        return lax.dot_general(
            diag, both, (((0,), (0,)), ((), ())), preferred_element_type=f32).astype(bf16)

    def keep(dst, q, value):
        dst[q * TILE:(q + 1) * TILE, :] = value

    with jax.named_scope("turn"):
        loads[1].wait()
        for q in range(couples):
            at = slice(q * TILE, (q + 1) * TILE)
            coef2[:, at] = coef[2 * q:2 * q + 2].reshape(2 * rank, rows).T

    def splat(flag, count):
        return jnp.full((count, TILE), jnp.where(flag, 1.0, 0.0), f32).astype(bf16)

    low = jnp.where(lax.broadcasted_iota(jnp.int32, (SUB, TILE), 1) < rank, 1.0, 0.0).astype(bf16)
    high = jnp.where(lax.broadcasted_iota(jnp.int32, (SUB, TILE), 1) < rank, 0.0, 1.0).astype(bf16)

    with jax.named_scope("lhs"):
        loads[0].wait()

        def place_of(s):
            bits = s % 2, (s // 2) % 2, s // 4
            same = [me if bit else 1 - me for bit, me in zip(bits, (c, x, y))]
            return same[0] * half_rows + (same[1] * 2 + same[2]) * part, same[0] * half_rows + 2 * shard + (same[2] * 2 + same[1]) * part

        places = [place_of(s) for s in range(2 * half_rows // shard)]
        for b in range(NBLK):
            for q in range(couples):
                at = slice(q * TILE, (q + 1) * TILE)
                m0, m1 = [splat(pao[h, 2 * q] == b, SUB) * low + splat(pao[h, 2 * q + 1] == b, SUB) * high for h in range(2)]
                for r in range(0, TILE, SUB):
                    s, inner = divmod(b * TILE + r, shard)
                    group, inner = divmod(inner, part)
                    dst = pl.ds(pl.multiple_of(places[s][group] + inner, SUB), SUB)
                    lhs[dst, at] = coef2[r:r + SUB, at] * m0 + coef2[TILE + r:TILE + r + SUB, at] * m1

    with jax.named_scope("mix"):
        loads[2].wait()
        for q in range(couples):
            keep(wei2, q, mixed(dens, q, coef[2 * q:2 * q + 2].reshape(2 * rank, rows)))

    def mix_integrals():
        for n in range(3, 7):
            loads[n].wait()
        for h in range(2):
            for n in range(pairs):
                labels[h * pairs + n] = aux[h, n] * ABPO + off[h, n]
        for q in range(couples):
            keep(tri2, q, mixed(amps, q, ints[2 * q:2 * q + 2].reshape(2 * rank, rows)))

    def build(t):
        kind, role, piece = TILES[t]

        for n in range(pairs):
            at = slice(n * rank, (n + 1) * rank)
            if kind == "aux":
                src, first = tri2, owner_of[role] * ABPO + 2 * piece
                names = [labels[h * pairs + n] for h in range(2)]
            else:
                src, first = wei2, 2 * piece
                names = [pao[h, n] for h in range(2)]
            low_part, high_part = src[at, 0:TILE], src[at, TILE:2 * TILE]
            for j in range(2):
                rhs[t % 2, at, j * TILE:(j + 1) * TILE] = (
                    low_part * splat(names[0] == first + j, rank) + high_part * splat(names[1] == first + j, rank))

    def product(t, half):
        return lax.dot_general(
            lhs[half * half_rows:(half + 1) * half_rows, :], rhs[t % 2], (((1,), (0,)), ((), ())),
            preferred_element_type=f32)

    count = len(TILES)
    stage1, stage2, to_owner, to_far, to_virt = count, 2 * count, 3 * count, 3 * count + 6, 3 * count + 7

    def make(t):
        with jax.named_scope(f"make{t}"):
            c_send[t] = product(t, 0).astype(bf16)
            if t == 0:
                pl.semaphore_wait(barrier, 6)
                send(c_send.at[t], c_recv.at[t], 0, t, core)
            own[t % 2] = product(t, 1)
            if t + 1 < count and t != 2:
                build(t + 1)
        if t:
            send(c_send.at[t], c_recv.at[t], 0, t, core)

    def first(t):
        with jax.named_scope(f"first{t}"):
            arrived(c_recv.at[t], t)

            def summed(lo):
                return own[t % 2, lo:lo + shard] + c_recv[t, lo:lo + shard].astype(f32)

            s1_send[t, 0:shard] = summed(0).astype(bf16)
            at = pl.ds(0, shard)
            send(s1_send.at[t, at], s1_recv.at[t, at], 1, stage1 + t, xdev)
            s1_send[t, shard:2 * shard] = summed(2 * shard).astype(bf16)
            at = pl.ds(shard, shard)
            send(s1_send.at[t, at], s1_recv.at[t, at], 1, stage1 + t, ydev)
            keep1[t, 0:shard] = summed(shard)
            keep1[t, shard:2 * shard] = summed(3 * shard)

    def second(t):
        with jax.named_scope(f"second{t}"):
            arrived(s1_recv.at[t], stage1 + t)
            for lo, dev in ((0, ydev), (part, xdev)):
                near = slice(2 * lo, 2 * lo + part)
                s2_send[t, lo:lo + part] = (keep1[t, near] + s1_recv[t, near].astype(f32)).astype(bf16)
                at = pl.ds(lo, part)
                send(s2_send.at[t, at], s2_recv.at[t, at], 2, stage2 + t, dev)
            for lo in (0, part):
                rest = slice(2 * lo + part, 2 * lo + shard)
                keep2[t, lo:lo + part] = keep1[t, rest] + s1_recv[t, rest].astype(f32)

    def third(t):
        kind, role, piece = TILES[t]
        with jax.named_scope(f"third{t}"):
            arrived(s2_recv.at[t], stage2 + t)
            if role == "early":
                arrived(p_recv.at[4 + piece], to_owner + 4 + piece)
            if role == "own":
                arrived(p_recv.at[piece], to_owner + piece)
                arrived(p_recv.at[2 + piece], to_owner + 2 + piece)
            total = keep2[t] + s2_recv[t].astype(f32)
            if kind == "virt":
                for j in range(2):
                    v_sum[2 * piece + j] = total[:, j * TILE:(j + 1) * TILE]
                if piece == 2:
                    f_send[...] = v_sum[blocks_of(flips[3])].astype(bf16)
                    send(f_send, f_recv, 4, to_far, (p, flips[1]))
            elif role == "own":
                gamma[:, piece * WIDE:(piece + 1) * WIDE] = (
                    total + p_recv[piece].astype(f32) + p_recv[2 + piece].astype(f32)) * scale
            else:
                flip = flip_of[role]
                if role != "far":
                    total = total + p_recv[4 + piece].astype(f32) * (flip - 1).astype(f32)
                n = 2 * flip - 2 + piece
                p_send[n] = total.astype(bf16)
                dev = flips[1] if role == "far" else owner_of[role]
                send(p_send.at[n], p_recv.at[n], 3, to_owner + n, (p, dev))

    def blocks_of(owner):
        return pl.ds(3 * (owner // 2) + owner % 2, 2)

    def virt_across():
        with jax.named_scope("virt_across"):
            arrived(f_recv, to_far)
            v_send[0] = v_sum[blocks_of(flips[1])].astype(bf16)
            v_send[1] = (v_sum[blocks_of(flips[2])] + f_recv[...].astype(f32)).astype(bf16)
            for role in ("early", "late"):
                n = flip_of[role] - 1
                send(v_send.at[n], v_recv.at[n], 5, to_virt + n, (p, owner_of[role]))

    def virt_out():
        with jax.named_scope("virt_out"):
            for n in range(2):
                arrived(v_recv.at[n], to_virt + n)
            total = v_sum[blocks_of(z)] + v_recv[0].astype(f32) + v_recv[1].astype(f32)
            strip = virt.shape[0]
            for j in range(2):
                flat[0:shard, j * TILE:(j + 1) * TILE] = total[j] * scale
            flat[shard:] = jnp.zeros((TILE - shard, WIDE), f32)
            turned[...] = flat[...].T
            virt[...] = turned[pl.ds(pl.multiple_of(z0 * (WIDE - strip), 8), strip), 0:shard]

    with jax.named_scope("pipeline"):
        build(0)
        for t in range(count + 5):
            if t < count:
                make(t)
            if t == 2:
                with jax.named_scope("mix_integrals"):
                    mix_integrals()
                    build(3)
            if 0 <= t - 1 < count:
                first(t - 1)
            if 0 <= t - 3 < count:
                second(t - 3)
            if 0 <= t - 5 < count:
                third(t - 5)
            if t == 9:
                virt_across()
            if t == 13:
                virt_out()
    for family, ref in enumerate((c_send, s1_send, s2_send, p_send, f_send, v_send)):
        pltpu.make_async_copy(ref, ref, send_sems.at[family]).wait()


def put_out(gamma, virt, gamma_out, virt_out, sems):
    copies = [pltpu.make_async_copy(gamma, gamma_out, sems.at[0]), pltpu.make_async_copy(virt, virt_out, sems.at[1])]
    for copy in copies:
        copy.start()
    for copy in copies:
        copy.wait()


def by_kernel(integrals, amplitudes, pno_density, pno_coef, pao_blocks, aux_slice, aux_offset):
    n_pair = lax.axis_size("pair")
    n_aux = lax.axis_size("aux")
    pairs, rows, rank = pno_coef.shape
    block = rows // pao_blocks.shape[1]
    ao_count = NBLK * block
    shard = ao_count // n_pair
    part = shard // 2
    width = pairs * rank
    count = len(TILES)
    scale = 1.0 / math.sqrt(pairs * n_pair)
    hbm = pl.BlockSpec(memory_space=pltpu.HBM)
    vmem = pl.BlockSpec(memory_space=pltpu.VMEM)

    def half(*dims):
        return pltpu.VMEM(dims, jnp.bfloat16)

    def full(*dims):
        return pltpu.VMEM(dims, jnp.float32)

    operands = (integrals.swapaxes(1, 2), amplitudes, pno_density, pno_coef.swapaxes(1, 2),
                pao_blocks.T, aux_slice.T, aux_offset.T)
    operands = tuple(pltpu.with_memory_space_constraint(a, pltpu.HBM) for a in operands)
    gamma, virt = pl.pallas_call(
        functools.partial(kernel, scale),
        out_shape=[
            jax.ShapeDtypeStruct((shard, ABPO * block), jnp.float32),
            jax.ShapeDtypeStruct((ao_count // n_aux, shard), jnp.float32),
        ],
        in_specs=[hbm] * 7,
        out_specs=[vmem] * 2,
        scratch_shapes=[half(*a.shape) for a in operands[:4]] + [pltpu.SMEM(a.shape, jnp.int32) for a in operands[4:]] + [
            pltpu.SMEM((2 * pairs,), jnp.int32),
            half(rows, width), half(width, rows), half(width, rows),
            half(8 * shard, width), half(2, width, WIDE), full(2, 4 * shard, WIDE),
            half(count, 4 * shard, WIDE), half(count, 4 * shard, WIDE)]
        + [half(count, 2 * shard, WIDE)] * 2 + [half(count, shard, WIDE)] * 2 + [
            full(count, 2 * shard, WIDE), full(count, shard, WIDE),
            half(6, shard, WIDE), half(6, shard, WIDE),
            half(2, shard, TILE), half(2, shard, TILE), half(2, 2, shard, TILE), half(2, 2, shard, TILE), full(NBLK, shard, TILE),
            full(TILE, WIDE), full(WIDE, TILE),
            pltpu.SemaphoreType.DMA((7,)),
            pltpu.SemaphoreType.DMA((SENDS,)),
            pltpu.SemaphoreType.DMA((RECVS,)),
        ],
        compiler_params=pltpu.CompilerParams(
            collective_id=0, has_side_effects=True, vmem_limit_bytes=36 * 1024 * 1024),
    )(*operands)
    gamma, virt = [pltpu.with_memory_space_constraint(a, pltpu.VMEM) for a in (gamma, virt)]
    gamma, virt = pl.pallas_call(
        put_out,
        out_shape=[jax.ShapeDtypeStruct(a.shape, a.dtype) for a in (gamma, virt)],
        in_specs=[vmem] * 2,
        out_specs=[hbm] * 2,
        scratch_shapes=[pltpu.SemaphoreType.DMA((2,))],
    )(gamma, virt)
    return gamma.T, virt


def on_device(*args):
    pairs, rows, rank = args[3].shape
    fits = lax.axis_size("pair") == 8 and lax.axis_size("aux") == 4 and pairs % 2 == 0 and 2 * rank == TILE
    fits = fits and rows == 2 * TILE and args[0].shape[1] == 2 * TILE
    return by_kernel(*args) if fits else by_collectives(*args)


def solution(mesh):
    in_specs = (
        P(("pair", "aux"), None, None),
        P(("pair", "aux"), None, None),
        P(("pair", "aux"), None, None),
        P(("pair", "aux"), None, None),
        P(("pair", "aux"), None),
        P(("pair", "aux"), None),
        P(("pair", "aux"), None),
    )
    out_specs = (P("aux", "pair"), P("aux", "pair"))
    return jax.shard_map(
        on_device, mesh=mesh, in_specs=in_specs, out_specs=out_specs, check_vma=False
    )
```

```python
import functools
import math

import jax
import jax.numpy as jnp
from jax import lax
from jax.experimental import pallas as pl
from jax.experimental.pallas import tpu as pltpu
from jax.sharding import PartitionSpec as P

NBLK = 6
ABPO = 4
MESH = pl.DeviceIdType.MESH
TILE = 128
SUB = 16


def by_collectives(integrals, amplitudes, pno_density, pno_coef, pao_blocks, aux_slice, aux_offset):
    n_pair = lax.axis_size("pair")
    n_aux = lax.axis_size("aux")
    pair_count, domain_rows, pno_rank = pno_coef.shape
    aux_dom = aux_slice.shape[1]
    pao_dom = pao_blocks.shape[1]
    pao_block = domain_rows // pao_dom
    aux_block = integrals.shape[1] // aux_dom
    ao_count = NBLK * pao_block
    capacity = max(2, 2 * pair_count * aux_dom // n_aux)
    out_scale = 1.0 / math.sqrt(pair_count * n_pair)
    slot_count = pair_count * aux_dom
    three_index = jnp.einsum(
        "pqr,prs->pqs", integrals, amplitudes, preferred_element_type=jnp.float32
    ).astype(jnp.bfloat16)
    owners = aux_slice.reshape(slot_count)
    owner_hot = (owners[:, None] == jnp.arange(n_aux, dtype=jnp.int32)[None, :]).astype(jnp.int32)
    before = jnp.cumsum(owner_hot, 0) - owner_hot
    slot_rank = jnp.sum(before * owner_hot, 1)
    target = owners * capacity + slot_rank
    routing = jnp.arange(n_aux * capacity, dtype=jnp.int32)[:, None] == target[None, :]
    labels = (
        jnp.concatenate(
            [aux_offset.reshape(slot_count, 1), jnp.repeat(pao_blocks, aux_dom, axis=0)], 1
        )
        + 1
    )
    label_buffer = (jnp.dot(routing.astype(jnp.int32), labels) - 1).reshape(
        n_aux, capacity, 1 + pao_dom
    )
    routing_bf = routing.astype(jnp.bfloat16)
    index_flat = three_index.reshape(slot_count, aux_block * pno_rank)
    index_buffer = jnp.dot(routing_bf, index_flat, preferred_element_type=jnp.float32).astype(
        jnp.bfloat16
    )
    index_buffer = index_buffer.reshape(n_aux, capacity, aux_block, pno_rank)
    pair_routing = (
        routing.reshape(n_aux * capacity, pair_count, aux_dom).sum(-1).astype(jnp.bfloat16)
    )
    coef_flat = pno_coef.reshape(pair_count, domain_rows * pno_rank)
    coef_buffer = jnp.dot(pair_routing, coef_flat, preferred_element_type=jnp.float32).astype(
        jnp.bfloat16
    )
    coef_buffer = coef_buffer.reshape(n_aux, capacity, domain_rows, pno_rank)
    index_part = lax.all_to_all(index_buffer, "aux", split_axis=0, concat_axis=0, tiled=True)
    coef_part = lax.all_to_all(coef_buffer, "aux", split_axis=0, concat_axis=0, tiled=True)
    label_part = lax.all_to_all(label_buffer, "aux", split_axis=0, concat_axis=0, tiled=True)
    back = jnp.einsum(
        "ncxr,ncyr->ncxy", index_part, coef_part, preferred_element_type=jnp.float32
    ).astype(jnp.bfloat16)
    got_labels = label_part
    received_count = n_aux * capacity
    pieces = back.reshape(received_count, aux_block, pao_dom, pao_block)
    got_labels = got_labels.reshape(received_count, 1 + pao_dom)
    offset_hot = got_labels[:, 0:1] == jnp.arange(ABPO, dtype=jnp.int32)[None, :]
    column_hot = got_labels[:, 1:, None] == jnp.arange(NBLK, dtype=jnp.int32)[None, None, :]
    placement = (offset_hot[:, None, :, None] & column_hot[:, :, None, :]).astype(jnp.bfloat16)
    gamma_part = jnp.einsum(
        "sxhy,shok->oxky", pieces, placement, preferred_element_type=jnp.float32
    )
    gamma_part = gamma_part.reshape(ABPO * aux_block, ao_count)
    aux_density = lax.psum_scatter(gamma_part, "pair", scatter_dimension=1, tiled=True) * out_scale
    weighted = jnp.einsum(
        "pyr,prs->pys", pno_coef, pno_density, preferred_element_type=jnp.float32
    ).astype(jnp.bfloat16)
    block_hot = (pao_blocks[:, :, None] == jnp.arange(NBLK, dtype=jnp.int32)[None, None, :]).astype(
        jnp.bfloat16
    )
    weighted_rows = jnp.einsum(
        "pak,paxr->kxpr",
        block_hot,
        weighted.reshape(pair_count, pao_dom, pao_block, pno_rank),
        preferred_element_type=jnp.float32,
    ).astype(jnp.bfloat16)
    weighted_rows = weighted_rows.reshape(ao_count, pair_count * pno_rank)
    coef_rows = jnp.einsum(
        "pak,paxr->kxpr",
        block_hot,
        pno_coef.reshape(pair_count, pao_dom, pao_block, pno_rank),
        preferred_element_type=jnp.float32,
    ).astype(jnp.bfloat16)
    coef_rows = coef_rows.reshape(ao_count, pair_count * pno_rank)
    virt_part = lax.dot_general(
        weighted_rows, coef_rows, (((1,), (1,)), ((), ())), preferred_element_type=jnp.float32
    )
    row_owned = lax.psum_scatter(virt_part, "aux", scatter_dimension=0, tiled=True)
    virtual_density = lax.psum_scatter(row_owned, "pair", scatter_dimension=1, tiled=True)
    return (aux_density, virtual_density * out_scale)


TILES = (("virt", 0, 0), ("virt", 0, 1), ("virt", 0, 2), ("aux", "far", 0), ("aux", "far", 1),
         ("aux", "early", 0), ("aux", "late", 0), ("aux", "early", 1), ("aux", "late", 1), ("aux", "own", 0), ("aux", "own", 1))
WIDE = 2 * TILE
RECVS = 3 * len(TILES) + 9
SENDS = 6


def kernel(scale, ints_in, amps_in, dens_in, coef_in, pao_in, aux_in, off_in, gamma, virt,
           ints, amps, dens, coef, pao, aux, off, labels, coef2, tri2, wei2, lhs, rhs, own, c_send, c_recv,
           s1_send, s1_recv, s2_send, s2_recv, keep1, keep2,
           p_send, p_recv, f_send, f_recv, v_send, v_recv, v_sum, flat, turned, load_sems, send_sems, recv_sems):
    pairs, rank, rows = coef.shape
    couples = pairs // 2
    shard = gamma.shape[0]
    part = shard // 2
    half_rows = 4 * shard
    f32, bf16 = jnp.float32, jnp.bfloat16
    p = lax.axis_index("pair")
    z = lax.axis_index("aux")
    c, x, y = p % 2, (p // 2) % 2, p // 4
    z0, z1 = z % 2, z // 2
    core = (p + 1 - 2 * c, z)
    xdev = (p + 2 - 4 * x, z)
    ydev = (p + 4 - 8 * y, z)
    flips = (z, z + 1 - 2 * z0, z + 2 - 4 * z1, 3 - z)
    at_end = 1 - z0 * (1 - z1)
    early, late = 1 + at_end, 2 - at_end
    flip_of = {"own": 0, "far": 3, "early": early, "late": late}
    owner_of = {"own": z, "far": flips[3], "early": flips[1] + at_end * (flips[2] - flips[1]),
                "late": flips[2] + at_end * (flips[1] - flips[2])}

    loads = [
        pltpu.make_async_copy(src, dst, load_sems.at[n])
        for n, (src, dst) in enumerate((
            (pao_in, pao), (coef_in, coef), (dens_in, dens), (amps_in, amps), (ints_in, ints), (aux_in, aux), (off_in, off)))
    ]
    for load in loads:
        load.start()

    barrier = pltpu.get_barrier_semaphore()
    for dev in (core, xdev, ydev) + tuple((p, flips[n]) for n in (1, 2, 3)):
        pl.semaphore_signal(barrier, inc=1, device_id=dev, device_id_type=MESH)

    def send(src, dst, family, slot, dev):
        pltpu.make_async_remote_copy(
            src_ref=src, dst_ref=dst, send_sem=send_sems.at[family], recv_sem=recv_sems.at[slot],
            device_id=dev, device_id_type=MESH).start()

    def arrived(ref, slot):
        pltpu.make_async_copy(ref, ref, recv_sems.at[slot]).wait()

    zero = jnp.zeros((rank, rank), bf16)

    def mixed(ref, q, both):
        diag = jnp.concatenate(
            [jnp.concatenate([ref[2 * q], zero], 1), jnp.concatenate([zero, ref[2 * q + 1]], 1)], 0)
        return lax.dot_general(
            diag, both, (((0,), (0,)), ((), ())), preferred_element_type=f32).astype(bf16)

    def keep(dst, q, value):
        dst[q * TILE:(q + 1) * TILE, :] = value

    with jax.named_scope("turn"):
        loads[1].wait()
        for q in range(couples):
            at = slice(q * TILE, (q + 1) * TILE)
            coef2[:, at] = coef[2 * q:2 * q + 2].reshape(2 * rank, rows).T

    def splat(flag, count):
        return jnp.full((count, TILE), jnp.where(flag, 1.0, 0.0), f32).astype(bf16)

    low = jnp.where(lax.broadcasted_iota(jnp.int32, (SUB, TILE), 1) < rank, 1.0, 0.0).astype(bf16)
    high = jnp.where(lax.broadcasted_iota(jnp.int32, (SUB, TILE), 1) < rank, 0.0, 1.0).astype(bf16)

    with jax.named_scope("lhs"):
        loads[0].wait()

        def place_of(s):
            bits = s % 2, (s // 2) % 2, s // 4
            same = [me if bit else 1 - me for bit, me in zip(bits, (c, x, y))]
            return same[0] * half_rows + (same[1] * 2 + same[2]) * part, same[0] * half_rows + 2 * shard + (same[2] * 2 + same[1]) * part

        places = [place_of(s) for s in range(2 * half_rows // shard)]
        for b in range(NBLK):
            for q in range(couples):
                at = slice(q * TILE, (q + 1) * TILE)
                m0, m1 = [splat(pao[h, 2 * q] == b, SUB) * low + splat(pao[h, 2 * q + 1] == b, SUB) * high for h in range(2)]
                for r in range(0, TILE, SUB):
                    s, inner = divmod(b * TILE + r, shard)
                    group, inner = divmod(inner, part)
                    dst = pl.ds(pl.multiple_of(places[s][group] + inner, SUB), SUB)
                    lhs[dst, at] = coef2[r:r + SUB, at] * m0 + coef2[TILE + r:TILE + r + SUB, at] * m1

    with jax.named_scope("mix"):
        loads[2].wait()
        for q in range(couples):
            keep(wei2, q, mixed(dens, q, coef[2 * q:2 * q + 2].reshape(2 * rank, rows)))

    def mix_integrals():
        for n in range(3, 7):
            loads[n].wait()
        for h in range(2):
            for n in range(pairs):
                labels[h * pairs + n] = aux[h, n] * ABPO + off[h, n]
        for q in range(couples):
            keep(tri2, q, mixed(amps, q, ints[2 * q:2 * q + 2].reshape(2 * rank, rows)))

    def build(t):
        kind, role, piece = TILES[t]

        for n in range(pairs):
            at = slice(n * rank, (n + 1) * rank)
            if kind == "aux":
                src, first = tri2, owner_of[role] * ABPO + 2 * piece
                names = [labels[h * pairs + n] for h in range(2)]
            else:
                src, first = wei2, 2 * piece
                names = [pao[h, n] for h in range(2)]
            low_part, high_part = src[at, 0:TILE], src[at, TILE:2 * TILE]
            for j in range(2):
                rhs[t % 2, at, j * TILE:(j + 1) * TILE] = (
                    low_part * splat(names[0] == first + j, rank) + high_part * splat(names[1] == first + j, rank))

    def product(t, half):
        return lax.dot_general(
            lhs[half * half_rows:(half + 1) * half_rows, :], rhs[t % 2], (((1,), (0,)), ((), ())),
            preferred_element_type=f32)

    count = len(TILES)
    stage1, stage2, to_owner, to_far, to_virt = count, 2 * count, 3 * count, 3 * count + 6, 3 * count + 7

    def make(t):
        with jax.named_scope(f"make{t}"):
            c_send[t] = product(t, 0).astype(bf16)
            if t == 0:
                pl.semaphore_wait(barrier, 6)
                send(c_send.at[t], c_recv.at[t], 0, t, core)
            own[t % 2] = product(t, 1)
            if t + 1 < count and t != 2:
                build(t + 1)
        if t:
            send(c_send.at[t], c_recv.at[t], 0, t, core)

    def first(t):
        with jax.named_scope(f"first{t}"):
            arrived(c_recv.at[t], t)

            def summed(lo):
                return own[t % 2, lo:lo + shard] + c_recv[t, lo:lo + shard].astype(f32)

            s1_send[t, 0:shard] = summed(0).astype(bf16)
            at = pl.ds(0, shard)
            send(s1_send.at[t, at], s1_recv.at[t, at], 1, stage1 + t, xdev)
            s1_send[t, shard:2 * shard] = summed(2 * shard).astype(bf16)
            at = pl.ds(shard, shard)
            send(s1_send.at[t, at], s1_recv.at[t, at], 1, stage1 + t, ydev)
            keep1[t, 0:shard] = summed(shard)
            keep1[t, shard:2 * shard] = summed(3 * shard)

    def second(t):
        with jax.named_scope(f"second{t}"):
            arrived(s1_recv.at[t], stage1 + t)
            for lo, dev in ((0, ydev), (part, xdev)):
                near = slice(2 * lo, 2 * lo + part)
                s2_send[t, lo:lo + part] = (keep1[t, near] + s1_recv[t, near].astype(f32)).astype(bf16)
                at = pl.ds(lo, part)
                send(s2_send.at[t, at], s2_recv.at[t, at], 2, stage2 + t, dev)
            for lo in (0, part):
                rest = slice(2 * lo + part, 2 * lo + shard)
                keep2[t, lo:lo + part] = keep1[t, rest] + s1_recv[t, rest].astype(f32)

    def third(t):
        kind, role, piece = TILES[t]
        with jax.named_scope(f"third{t}"):
            arrived(s2_recv.at[t], stage2 + t)
            if role == "early":
                arrived(p_recv.at[4 + piece], to_owner + 4 + piece)
            if role == "own":
                arrived(p_recv.at[piece], to_owner + piece)
                arrived(p_recv.at[2 + piece], to_owner + 2 + piece)
            total = keep2[t] + s2_recv[t].astype(f32)
            if kind == "virt":
                for j in range(2):
                    v_sum[2 * piece + j] = total[:, j * TILE:(j + 1) * TILE]
                if piece == 2:
                    f_send[...] = v_sum[blocks_of(flips[3])].astype(bf16)
                    send(f_send, f_recv, 4, to_far, (p, flips[1]))
            elif role == "own":
                gamma[:, piece * WIDE:(piece + 1) * WIDE] = (
                    total + p_recv[piece].astype(f32) + p_recv[2 + piece].astype(f32)) * scale
            else:
                flip = flip_of[role]
                if role != "far":
                    total = total + p_recv[4 + piece].astype(f32) * (flip - 1).astype(f32)
                n = 2 * flip - 2 + piece
                p_send[n] = total.astype(bf16)
                dev = flips[1] if role == "far" else owner_of[role]
                send(p_send.at[n], p_recv.at[n], 3, to_owner + n, (p, dev))

    def blocks_of(owner):
        return pl.ds(3 * (owner // 2) + owner % 2, 2)

    def virt_across():
        with jax.named_scope("virt_across"):
            arrived(f_recv, to_far)
            v_send[0] = v_sum[blocks_of(flips[1])].astype(bf16)
            v_send[1] = (v_sum[blocks_of(flips[2])] + f_recv[...].astype(f32)).astype(bf16)
            for role in ("early", "late"):
                n = flip_of[role] - 1
                send(v_send.at[n], v_recv.at[n], 5, to_virt + n, (p, owner_of[role]))

    def virt_out():
        with jax.named_scope("virt_out"):
            for n in range(2):
                arrived(v_recv.at[n], to_virt + n)
            total = v_sum[blocks_of(z)] + v_recv[0].astype(f32) + v_recv[1].astype(f32)
            strip = virt.shape[0]
            for j in range(2):
                flat[0:shard, j * TILE:(j + 1) * TILE] = total[j] * scale
            flat[shard:] = jnp.zeros((TILE - shard, WIDE), f32)
            turned[...] = flat[...].T
            virt[...] = turned[pl.ds(pl.multiple_of(z0 * (WIDE - strip), 8), strip), 0:shard]

    with jax.named_scope("pipeline"):
        build(0)
        for t in range(count + 5):
            if t < count:
                make(t)
            if t == 2:
                with jax.named_scope("mix_integrals"):
                    mix_integrals()
                    build(3)
            if 0 <= t - 1 < count:
                first(t - 1)
            if 0 <= t - 3 < count:
                second(t - 3)
            if 0 <= t - 5 < count:
                third(t - 5)
            if t == 9:
                virt_across()
            if t == 13:
                virt_out()
    for family, ref in enumerate((c_send, s1_send, s2_send, p_send, f_send, v_send)):
        pltpu.make_async_copy(ref, ref, send_sems.at[family]).wait()


def put_out(gamma, virt, gamma_out, virt_out, sems):
    copies = [pltpu.make_async_copy(gamma, gamma_out, sems.at[0]), pltpu.make_async_copy(virt, virt_out, sems.at[1])]
    for copy in copies:
        copy.start()
    for copy in copies:
        copy.wait()


def by_kernel(integrals, amplitudes, pno_density, pno_coef, pao_blocks, aux_slice, aux_offset):
    n_pair = lax.axis_size("pair")
    n_aux = lax.axis_size("aux")
    pairs, rows, rank = pno_coef.shape
    block = rows // pao_blocks.shape[1]
    ao_count = NBLK * block
    shard = ao_count // n_pair
    part = shard // 2
    width = pairs * rank
    count = len(TILES)
    scale = 1.0 / math.sqrt(pairs * n_pair)
    hbm = pl.BlockSpec(memory_space=pltpu.HBM)
    vmem = pl.BlockSpec(memory_space=pltpu.VMEM)

    def half(*dims):
        return pltpu.VMEM(dims, jnp.bfloat16)

    def full(*dims):
        return pltpu.VMEM(dims, jnp.float32)

    operands = (integrals.swapaxes(1, 2), amplitudes, pno_density, pno_coef.swapaxes(1, 2),
                pao_blocks.T, aux_slice.T, aux_offset.T)
    operands = tuple(pltpu.with_memory_space_constraint(a, pltpu.HBM) for a in operands)
    gamma, virt = pl.pallas_call(
        functools.partial(kernel, scale),
        out_shape=[
            jax.ShapeDtypeStruct((shard, ABPO * block), jnp.float32),
            jax.ShapeDtypeStruct((ao_count // n_aux, shard), jnp.float32),
        ],
        in_specs=[hbm] * 7,
        out_specs=[vmem] * 2,
        scratch_shapes=[half(*a.shape) for a in operands[:4]] + [pltpu.SMEM(a.shape, jnp.int32) for a in operands[4:]] + [
            pltpu.SMEM((2 * pairs,), jnp.int32),
            half(rows, width), half(width, rows), half(width, rows),
            half(8 * shard, width), half(2, width, WIDE), full(2, 4 * shard, WIDE),
            half(count, 4 * shard, WIDE), half(count, 4 * shard, WIDE)]
        + [half(count, 2 * shard, WIDE)] * 2 + [half(count, shard, WIDE)] * 2 + [
            full(count, 2 * shard, WIDE), full(count, shard, WIDE),
            half(6, shard, WIDE), half(6, shard, WIDE),
            half(2, shard, TILE), half(2, shard, TILE), half(2, 2, shard, TILE), half(2, 2, shard, TILE), full(NBLK, shard, TILE),
            full(TILE, WIDE), full(WIDE, TILE),
            pltpu.SemaphoreType.DMA((7,)),
            pltpu.SemaphoreType.DMA((SENDS,)),
            pltpu.SemaphoreType.DMA((RECVS,)),
        ],
        compiler_params=pltpu.CompilerParams(
            collective_id=0, has_side_effects=True, vmem_limit_bytes=36 * 1024 * 1024),
    )(*operands)
    gamma, virt = [pltpu.with_memory_space_constraint(a, pltpu.VMEM) for a in (gamma, virt)]
    gamma, virt = pl.pallas_call(
        put_out,
        out_shape=[jax.ShapeDtypeStruct(a.shape, a.dtype) for a in (gamma, virt)],
        in_specs=[vmem] * 2,
        out_specs=[hbm] * 2,
        scratch_shapes=[pltpu.SemaphoreType.DMA((2,))],
    )(gamma, virt)
    return gamma.T, virt


def on_device(*args):
    pairs, rows, rank = args[3].shape
    fits = lax.axis_size("pair") == 8 and lax.axis_size("aux") == 4 and pairs % 2 == 0 and 2 * rank == TILE
    fits = fits and rows == 2 * TILE and args[0].shape[1] == 2 * TILE
    return by_kernel(*args) if fits else by_collectives(*args)


def solution(mesh):
    in_specs = (
        P(("pair", "aux"), None, None),
        P(("pair", "aux"), None, None),
        P(("pair", "aux"), None, None),
        P(("pair", "aux"), None, None),
        P(("pair", "aux"), None),
        P(("pair", "aux"), None),
        P(("pair", "aux"), None),
    )
    out_specs = (P("aux", "pair"), P("aux", "pair"))
    return jax.shard_map(
        on_device, mesh=mesh, in_specs=in_specs, out_specs=out_specs, check_vma=False
    )
```

```python
import functools
import math

import jax
import jax.numpy as jnp
from jax import lax
from jax.experimental import pallas as pl
from jax.experimental.pallas import tpu as pltpu
from jax.sharding import PartitionSpec as P

NBLK = 6
ABPO = 4
MESH = pl.DeviceIdType.MESH
TILE = 128
SUB = 16


def by_collectives(integrals, amplitudes, pno_density, pno_coef, pao_blocks, aux_slice, aux_offset):
    n_pair = lax.axis_size("pair")
    n_aux = lax.axis_size("aux")
    pair_count, domain_rows, pno_rank = pno_coef.shape
    aux_dom = aux_slice.shape[1]
    pao_dom = pao_blocks.shape[1]
    pao_block = domain_rows // pao_dom
    aux_block = integrals.shape[1] // aux_dom
    ao_count = NBLK * pao_block
    capacity = max(2, 2 * pair_count * aux_dom // n_aux)
    out_scale = 1.0 / math.sqrt(pair_count * n_pair)
    slot_count = pair_count * aux_dom
    three_index = jnp.einsum(
        "pqr,prs->pqs", integrals, amplitudes, preferred_element_type=jnp.float32
    ).astype(jnp.bfloat16)
    owners = aux_slice.reshape(slot_count)
    owner_hot = (owners[:, None] == jnp.arange(n_aux, dtype=jnp.int32)[None, :]).astype(jnp.int32)
    before = jnp.cumsum(owner_hot, 0) - owner_hot
    slot_rank = jnp.sum(before * owner_hot, 1)
    target = owners * capacity + slot_rank
    routing = jnp.arange(n_aux * capacity, dtype=jnp.int32)[:, None] == target[None, :]
    labels = (
        jnp.concatenate(
            [aux_offset.reshape(slot_count, 1), jnp.repeat(pao_blocks, aux_dom, axis=0)], 1
        )
        + 1
    )
    label_buffer = (jnp.dot(routing.astype(jnp.int32), labels) - 1).reshape(
        n_aux, capacity, 1 + pao_dom
    )
    routing_bf = routing.astype(jnp.bfloat16)
    index_flat = three_index.reshape(slot_count, aux_block * pno_rank)
    index_buffer = jnp.dot(routing_bf, index_flat, preferred_element_type=jnp.float32).astype(
        jnp.bfloat16
    )
    index_buffer = index_buffer.reshape(n_aux, capacity, aux_block, pno_rank)
    pair_routing = (
        routing.reshape(n_aux * capacity, pair_count, aux_dom).sum(-1).astype(jnp.bfloat16)
    )
    coef_flat = pno_coef.reshape(pair_count, domain_rows * pno_rank)
    coef_buffer = jnp.dot(pair_routing, coef_flat, preferred_element_type=jnp.float32).astype(
        jnp.bfloat16
    )
    coef_buffer = coef_buffer.reshape(n_aux, capacity, domain_rows, pno_rank)
    index_part = lax.all_to_all(index_buffer, "aux", split_axis=0, concat_axis=0, tiled=True)
    coef_part = lax.all_to_all(coef_buffer, "aux", split_axis=0, concat_axis=0, tiled=True)
    label_part = lax.all_to_all(label_buffer, "aux", split_axis=0, concat_axis=0, tiled=True)
    back = jnp.einsum(
        "ncxr,ncyr->ncxy", index_part, coef_part, preferred_element_type=jnp.float32
    ).astype(jnp.bfloat16)
    got_labels = label_part
    received_count = n_aux * capacity
    pieces = back.reshape(received_count, aux_block, pao_dom, pao_block)
    got_labels = got_labels.reshape(received_count, 1 + pao_dom)
    offset_hot = got_labels[:, 0:1] == jnp.arange(ABPO, dtype=jnp.int32)[None, :]
    column_hot = got_labels[:, 1:, None] == jnp.arange(NBLK, dtype=jnp.int32)[None, None, :]
    placement = (offset_hot[:, None, :, None] & column_hot[:, :, None, :]).astype(jnp.bfloat16)
    gamma_part = jnp.einsum(
        "sxhy,shok->oxky", pieces, placement, preferred_element_type=jnp.float32
    )
    gamma_part = gamma_part.reshape(ABPO * aux_block, ao_count)
    aux_density = lax.psum_scatter(gamma_part, "pair", scatter_dimension=1, tiled=True) * out_scale
    weighted = jnp.einsum(
        "pyr,prs->pys", pno_coef, pno_density, preferred_element_type=jnp.float32
    ).astype(jnp.bfloat16)
    block_hot = (pao_blocks[:, :, None] == jnp.arange(NBLK, dtype=jnp.int32)[None, None, :]).astype(
        jnp.bfloat16
    )
    weighted_rows = jnp.einsum(
        "pak,paxr->kxpr",
        block_hot,
        weighted.reshape(pair_count, pao_dom, pao_block, pno_rank),
        preferred_element_type=jnp.float32,
    ).astype(jnp.bfloat16)
    weighted_rows = weighted_rows.reshape(ao_count, pair_count * pno_rank)
    coef_rows = jnp.einsum(
        "pak,paxr->kxpr",
        block_hot,
        pno_coef.reshape(pair_count, pao_dom, pao_block, pno_rank),
        preferred_element_type=jnp.float32,
    ).astype(jnp.bfloat16)
    coef_rows = coef_rows.reshape(ao_count, pair_count * pno_rank)
    virt_part = lax.dot_general(
        weighted_rows, coef_rows, (((1,), (1,)), ((), ())), preferred_element_type=jnp.float32
    )
    row_owned = lax.psum_scatter(virt_part, "aux", scatter_dimension=0, tiled=True)
    virtual_density = lax.psum_scatter(row_owned, "pair", scatter_dimension=1, tiled=True)
    return (aux_density, virtual_density * out_scale)


TILES = (("virt", 0, 0), ("virt", 0, 1), ("virt", 0, 2), ("aux", "far", 0), ("aux", "far", 1),
         ("aux", "early", 0), ("aux", "late", 0), ("aux", "early", 1), ("aux", "late", 1), ("aux", "own", 0), ("aux", "own", 1))
WIDE = 2 * TILE
RECVS = 3 * len(TILES) + 9
SENDS = 6


def kernel(scale, ints_in, amps_in, dens_in, coef_in, pao_in, aux_in, off_in, gamma, virt,
           ints, amps, dens, coef, pao, aux, off, labels, coef2, tri2, wei2, lhs, rhs, own, c_send, c_recv,
           s1_send, s1_recv, s2_send, s2_recv, keep1, keep2,
           p_send, p_recv, f_send, f_recv, v_send, v_recv, v_sum, flat, turned, load_sems, send_sems, recv_sems):
    pairs, rank, rows = coef.shape
    couples = pairs // 2
    shard = gamma.shape[0]
    part = shard // 2
    half_rows = 4 * shard
    f32, bf16 = jnp.float32, jnp.bfloat16
    p = lax.axis_index("pair")
    z = lax.axis_index("aux")
    c, x, y = p % 2, (p // 2) % 2, p // 4
    z0, z1 = z % 2, z // 2
    core = (p + 1 - 2 * c, z)
    xdev = (p + 2 - 4 * x, z)
    ydev = (p + 4 - 8 * y, z)
    flips = (z, z + 1 - 2 * z0, z + 2 - 4 * z1, 3 - z)
    at_end = 1 - z0 * (1 - z1)
    early, late = 1 + at_end, 2 - at_end
    flip_of = {"own": 0, "far": 3, "early": early, "late": late}
    owner_of = {"own": z, "far": flips[3], "early": flips[1] + at_end * (flips[2] - flips[1]),
                "late": flips[2] + at_end * (flips[1] - flips[2])}

    loads = [
        pltpu.make_async_copy(src, dst, load_sems.at[n])
        for n, (src, dst) in enumerate((
            (pao_in, pao), (coef_in, coef), (dens_in, dens), (amps_in, amps), (ints_in, ints), (aux_in, aux), (off_in, off)))
    ]
    for load in loads:
        load.start()

    barrier = pltpu.get_barrier_semaphore()
    for dev in (core, xdev, ydev) + tuple((p, flips[n]) for n in (1, 2, 3)):
        pl.semaphore_signal(barrier, inc=1, device_id=dev, device_id_type=MESH)

    def send(src, dst, family, slot, dev):
        pltpu.make_async_remote_copy(
            src_ref=src, dst_ref=dst, send_sem=send_sems.at[family], recv_sem=recv_sems.at[slot],
            device_id=dev, device_id_type=MESH).start()

    def arrived(ref, slot):
        pltpu.make_async_copy(ref, ref, recv_sems.at[slot]).wait()

    zero = jnp.zeros((rank, rank), bf16)

    def mixed(ref, q, both):
        diag = jnp.concatenate(
            [jnp.concatenate([ref[2 * q], zero], 1), jnp.concatenate([zero, ref[2 * q + 1]], 1)], 0)
        return lax.dot_general(
            diag, both, (((0,), (0,)), ((), ())), preferred_element_type=f32).astype(bf16)

    def keep(dst, q, value):
        dst[q * TILE:(q + 1) * TILE, :] = value

    with jax.named_scope("turn"):
        loads[1].wait()
        for q in range(couples):
            at = slice(q * TILE, (q + 1) * TILE)
            coef2[:, at] = coef[2 * q:2 * q + 2].reshape(2 * rank, rows).T

    def splat(flag, count):
        return jnp.full((count, TILE), jnp.where(flag, 1.0, 0.0), f32).astype(bf16)

    low = jnp.where(lax.broadcasted_iota(jnp.int32, (SUB, TILE), 1) < rank, 1.0, 0.0).astype(bf16)
    high = jnp.where(lax.broadcasted_iota(jnp.int32, (SUB, TILE), 1) < rank, 0.0, 1.0).astype(bf16)

    with jax.named_scope("lhs"):
        loads[0].wait()

        def place_of(s):
            bits = s % 2, (s // 2) % 2, s // 4
            same = [me if bit else 1 - me for bit, me in zip(bits, (c, x, y))]
            return same[0] * half_rows + (same[1] * 2 + same[2]) * part, same[0] * half_rows + 2 * shard + (same[2] * 2 + same[1]) * part

        places = [place_of(s) for s in range(2 * half_rows // shard)]
        for b in range(NBLK):
            for q in range(couples):
                at = slice(q * TILE, (q + 1) * TILE)
                m0, m1 = [splat(pao[h, 2 * q] == b, SUB) * low + splat(pao[h, 2 * q + 1] == b, SUB) * high for h in range(2)]
                for r in range(0, TILE, SUB):
                    s, inner = divmod(b * TILE + r, shard)
                    group, inner = divmod(inner, part)
                    dst = pl.ds(pl.multiple_of(places[s][group] + inner, SUB), SUB)
                    lhs[dst, at] = coef2[r:r + SUB, at] * m0 + coef2[TILE + r:TILE + r + SUB, at] * m1

    with jax.named_scope("mix"):
        loads[2].wait()
        for q in range(couples):
            keep(wei2, q, mixed(dens, q, coef[2 * q:2 * q + 2].reshape(2 * rank, rows)))

    def mix_integrals():
        for n in range(3, 7):
            loads[n].wait()
        for h in range(2):
            for n in range(pairs):
                labels[h * pairs + n] = aux[h, n] * ABPO + off[h, n]
        for q in range(couples):
            keep(tri2, q, mixed(amps, q, ints[2 * q:2 * q + 2].reshape(2 * rank, rows)))

    def build(t):
        kind, role, piece = TILES[t]

        for n in range(pairs):
            at = slice(n * rank, (n + 1) * rank)
            if kind == "aux":
                src, first = tri2, owner_of[role] * ABPO + 2 * piece
                names = [labels[h * pairs + n] for h in range(2)]
            else:
                src, first = wei2, 2 * piece
                names = [pao[h, n] for h in range(2)]
            low_part, high_part = src[at, 0:TILE], src[at, TILE:2 * TILE]
            for j in range(2):
                rhs[t % 2, at, j * TILE:(j + 1) * TILE] = (
                    low_part * splat(names[0] == first + j, rank) + high_part * splat(names[1] == first + j, rank))

    def product(t, half):
        return lax.dot_general(
            lhs[half * half_rows:(half + 1) * half_rows, :], rhs[t % 2], (((1,), (0,)), ((), ())),
            preferred_element_type=f32)

    count = len(TILES)
    stage1, stage2, to_owner, to_far, to_virt = count, 2 * count, 3 * count, 3 * count + 6, 3 * count + 7

    def make(t):
        with jax.named_scope(f"make{t}"):
            c_send[t] = product(t, 0).astype(bf16)
            if t == 0:
                pl.semaphore_wait(barrier, 6)
                send(c_send.at[t], c_recv.at[t], 0, t, core)
            own[t % 2] = product(t, 1)
            if t + 1 < count and t != 2:
                build(t + 1)
        if t:
            send(c_send.at[t], c_recv.at[t], 0, t, core)

    def first(t):
        with jax.named_scope(f"first{t}"):
            arrived(c_recv.at[t], t)

            def summed(lo):
                return own[t % 2, lo:lo + shard] + c_recv[t, lo:lo + shard].astype(f32)

            s1_send[t, 0:shard] = summed(0).astype(bf16)
            at = pl.ds(0, shard)
            send(s1_send.at[t, at], s1_recv.at[t, at], 1, stage1 + t, xdev)
            s1_send[t, shard:2 * shard] = summed(2 * shard).astype(bf16)
            at = pl.ds(shard, shard)
            send(s1_send.at[t, at], s1_recv.at[t, at], 1, stage1 + t, ydev)
            keep1[t, 0:shard] = summed(shard)
            keep1[t, shard:2 * shard] = summed(3 * shard)

    def second(t):
        with jax.named_scope(f"second{t}"):
            arrived(s1_recv.at[t], stage1 + t)
            for lo, dev in ((0, ydev), (part, xdev)):
                near = slice(2 * lo, 2 * lo + part)
                s2_send[t, lo:lo + part] = (keep1[t, near] + s1_recv[t, near].astype(f32)).astype(bf16)
                at = pl.ds(lo, part)
                send(s2_send.at[t, at], s2_recv.at[t, at], 2, stage2 + t, dev)
            for lo in (0, part):
                rest = slice(2 * lo + part, 2 * lo + shard)
                keep2[t, lo:lo + part] = keep1[t, rest] + s1_recv[t, rest].astype(f32)

    def third(t):
        kind, role, piece = TILES[t]
        with jax.named_scope(f"third{t}"):
            arrived(s2_recv.at[t], stage2 + t)
            if role == "early":
                arrived(p_recv.at[4 + piece], to_owner + 4 + piece)
            if role == "own":
                arrived(p_recv.at[piece], to_owner + piece)
                arrived(p_recv.at[2 + piece], to_owner + 2 + piece)
            total = keep2[t] + s2_recv[t].astype(f32)
            if kind == "virt":
                for j in range(2):
                    v_sum[2 * piece + j] = total[:, j * TILE:(j + 1) * TILE]
                if piece == 2:
                    f_send[...] = v_sum[blocks_of(flips[3])].astype(bf16)
                    send(f_send, f_recv, 4, to_far, (p, flips[1]))
            elif role == "own":
                gamma[:, piece * WIDE:(piece + 1) * WIDE] = (
                    total + p_recv[piece].astype(f32) + p_recv[2 + piece].astype(f32)) * scale
            else:
                flip = flip_of[role]
                if role != "far":
                    total = total + p_recv[4 + piece].astype(f32) * (flip - 1).astype(f32)
                n = 2 * flip - 2 + piece
                p_send[n] = total.astype(bf16)
                dev = flips[1] if role == "far" else owner_of[role]
                send(p_send.at[n], p_recv.at[n], 3, to_owner + n, (p, dev))

    def blocks_of(owner):
        return pl.ds(3 * (owner // 2) + owner % 2, 2)

    def virt_across():
        with jax.named_scope("virt_across"):
            arrived(f_recv, to_far)
            v_send[0] = v_sum[blocks_of(flips[1])].astype(bf16)
            v_send[1] = (v_sum[blocks_of(flips[2])] + f_recv[...].astype(f32)).astype(bf16)
            for role in ("early", "late"):
                n = flip_of[role] - 1
                send(v_send.at[n], v_recv.at[n], 5, to_virt + n, (p, owner_of[role]))

    def virt_out():
        with jax.named_scope("virt_out"):
            for n in range(2):
                arrived(v_recv.at[n], to_virt + n)
            total = v_sum[blocks_of(z)] + v_recv[0].astype(f32) + v_recv[1].astype(f32)
            strip = virt.shape[0]
            for j in range(2):
                flat[0:shard, j * TILE:(j + 1) * TILE] = total[j] * scale
            flat[shard:] = jnp.zeros((TILE - shard, WIDE), f32)
            turned[...] = flat[...].T
            virt[...] = turned[pl.ds(pl.multiple_of(z0 * (WIDE - strip), 8), strip), 0:shard]

    with jax.named_scope("pipeline"):
        build(0)
        for t in range(count + 5):
            if t < count:
                make(t)
            if 0 <= t - 1 < count:
                first(t - 1)
            if t == 2:
                with jax.named_scope("mix_integrals"):
                    mix_integrals()
                    build(3)
            if 0 <= t - 3 < count:
                second(t - 3)
            if 0 <= t - 5 < count:
                third(t - 5)
            if t == 9:
                virt_across()
            if t == 13:
                virt_out()
    for family, ref in enumerate((c_send, s1_send, s2_send, p_send, f_send, v_send)):
        pltpu.make_async_copy(ref, ref, send_sems.at[family]).wait()


def put_out(gamma, virt, gamma_out, virt_out, sems):
    copies = [pltpu.make_async_copy(gamma, gamma_out, sems.at[0]), pltpu.make_async_copy(virt, virt_out, sems.at[1])]
    for copy in copies:
        copy.start()
    for copy in copies:
        copy.wait()


def by_kernel(integrals, amplitudes, pno_density, pno_coef, pao_blocks, aux_slice, aux_offset):
    n_pair = lax.axis_size("pair")
    n_aux = lax.axis_size("aux")
    pairs, rows, rank = pno_coef.shape
    block = rows // pao_blocks.shape[1]
    ao_count = NBLK * block
    shard = ao_count // n_pair
    part = shard // 2
    width = pairs * rank
    count = len(TILES)
    scale = 1.0 / math.sqrt(pairs * n_pair)
    hbm = pl.BlockSpec(memory_space=pltpu.HBM)
    vmem = pl.BlockSpec(memory_space=pltpu.VMEM)

    def half(*dims):
        return pltpu.VMEM(dims, jnp.bfloat16)

    def full(*dims):
        return pltpu.VMEM(dims, jnp.float32)

    operands = (integrals.swapaxes(1, 2), amplitudes, pno_density, pno_coef.swapaxes(1, 2),
                pao_blocks.T, aux_slice.T, aux_offset.T)
    operands = tuple(pltpu.with_memory_space_constraint(a, pltpu.HBM) for a in operands)
    gamma, virt = pl.pallas_call(
        functools.partial(kernel, scale),
        out_shape=[
            jax.ShapeDtypeStruct((shard, ABPO * block), jnp.float32),
            jax.ShapeDtypeStruct((ao_count // n_aux, shard), jnp.float32),
        ],
        in_specs=[hbm] * 7,
        out_specs=[vmem] * 2,
        scratch_shapes=[half(*a.shape) for a in operands[:4]] + [pltpu.SMEM(a.shape, jnp.int32) for a in operands[4:]] + [
            pltpu.SMEM((2 * pairs,), jnp.int32),
            half(rows, width), half(width, rows), half(width, rows),
            half(8 * shard, width), half(2, width, WIDE), full(2, 4 * shard, WIDE),
            half(count, 4 * shard, WIDE), half(count, 4 * shard, WIDE)]
        + [half(count, 2 * shard, WIDE)] * 2 + [half(count, shard, WIDE)] * 2 + [
            full(count, 2 * shard, WIDE), full(count, shard, WIDE),
            half(6, shard, WIDE), half(6, shard, WIDE),
            half(2, shard, TILE), half(2, shard, TILE), half(2, 2, shard, TILE), half(2, 2, shard, TILE), full(NBLK, shard, TILE),
            full(TILE, WIDE), full(WIDE, TILE),
            pltpu.SemaphoreType.DMA((7,)),
            pltpu.SemaphoreType.DMA((SENDS,)),
            pltpu.SemaphoreType.DMA((RECVS,)),
        ],
        compiler_params=pltpu.CompilerParams(
            collective_id=0, has_side_effects=True, vmem_limit_bytes=36 * 1024 * 1024),
    )(*operands)
    gamma, virt = [pltpu.with_memory_space_constraint(a, pltpu.VMEM) for a in (gamma, virt)]
    gamma, virt = pl.pallas_call(
        put_out,
        out_shape=[jax.ShapeDtypeStruct(a.shape, a.dtype) for a in (gamma, virt)],
        in_specs=[vmem] * 2,
        out_specs=[hbm] * 2,
        scratch_shapes=[pltpu.SemaphoreType.DMA((2,))],
    )(gamma, virt)
    return gamma.T, virt


def on_device(*args):
    pairs, rows, rank = args[3].shape
    fits = lax.axis_size("pair") == 8 and lax.axis_size("aux") == 4 and pairs % 2 == 0 and 2 * rank == TILE
    fits = fits and rows == 2 * TILE and args[0].shape[1] == 2 * TILE
    return by_kernel(*args) if fits else by_collectives(*args)


def solution(mesh):
    in_specs = (
        P(("pair", "aux"), None, None),
        P(("pair", "aux"), None, None),
        P(("pair", "aux"), None, None),
        P(("pair", "aux"), None, None),
        P(("pair", "aux"), None),
        P(("pair", "aux"), None),
        P(("pair", "aux"), None),
    )
    out_specs = (P("aux", "pair"), P("aux", "pair"))
    return jax.shard_map(
        on_device, mesh=mesh, in_specs=in_specs, out_specs=out_specs, check_vma=False
    )
```
